128 devices in a mesh: section: 2 (over core), tp: 4 (over x), pool: 16 (over z, y).
Axes of the slice: x: 4, y: 4, z: 4, core: 2. Of those that a mesh axis runs over, the one named last changes fastest.
Arguments:
- hidden: bfloat16 [2, 16, 128, 8192], P('section', 'pool', None, 'tp'), may hold values from -6 to 6
- queries: bfloat16 [2, 16, 16, 8, 64, 128], P('section', 'pool', None, None, 'tp'), may hold values from -450 to 450, as said below
- window_key_value: bfloat16 [2, 16, 16, 2, 8, 8, 128], P('section', 'pool', None, None, 'tp'), may hold values from -12 to 12
- cached_key_value: bfloat16 [2, 16, 128, 2, 8, 64, 128], P('section', 'pool', None, None, 'tp'), may hold values from -12 to 12
- cached_length: int32 [2, 16, 16], P('section', 'pool'), may hold values from 1 to 1024, 6144 in all within a row
- request_page_table: int32 [2, 16, 16, 16], P('section', 'pool'), may hold values from 0 to 127
- request_adapter: int32 [2, 16, 16], replicated, may hold values from 0 to 127, as said below
- layer_page_slot: int32 [256], replicated, may hold values from 0 to 255, as said below
- wo: bfloat16 [2, 8192, 8192], P('section', 'tp'), may hold values from -0.09375 to 0.09375
- adapter_down: bfloat16 [256, 64, 8192], P(('section', 'pool'), None, 'tp'), may hold values from -0.0625 to 0.0625
- adapter_up: bfloat16 [256, 64, 8192], P(('section', 'pool'), None, 'tp'), may hold values from -0.75 to 0.75
Outputs:
- next_hidden: bfloat16 [2, 16, 128, 8192], P('section', 'pool', None, 'tp')
The draws below stay inside these ranges and needn't reach their ends.
Inputs may be any that keep to these rules, and one draw needn't show every extreme that they name: `queries`: queries of order one; some entries far larger in the hidden draw. `request_page_table`: several requests may name the same cache page; entries past a request's length are read but excluded. `cached_length`: each request of a device has 1 to 1024 cached positions. `layer_page_slot`: the adapters of layer s occupy slots s * 128 to (s + 1) * 128 - 1, each slot once; slot q lies on the index q // 8 of section and pool taken together, section first, so layer s's pages sit on section s. `request_adapter`: up to all 16 requests of a pool group may use adapters held on one pool index, and one pool index may serve every request of its section.
All inputs are finite; a program needn't handle non-finite values.
Results may differ from the reference program's by a relative error of at most 0.009.
Values may be sent and summed in bfloat16 or wider, within the bound.
A program may use at most 192 MiB of HBM per device.

```python
import math
import jax
import jax.numpy as jnp
import numpy as np
from jax import lax

MODEL_WIDTH = 8192
QUERY_HEADS = 64
KV_HEADS = 8
HEAD_WIDTH = 128
ADAPTER_RANK = 64
PAGE_TOK = 64
WINDOW_TOKENS = 8
GROUP_REQUESTS = 16
MAX_PAGES = 16
CACHE_PAGES = 128
PAGES_DEV = 8
ADAPTER_COUNT = 128
N_SECTION = 2
N_POOL = 16


def draw_queries(key, part):
    first_key = jax.random.fold_in(key, 11)
    array_shape = (N_SECTION, N_POOL, GROUP_REQUESTS, WINDOW_TOKENS, QUERY_HEADS, HEAD_WIDTH)
    values = jnp.clip(jax.random.normal(first_key, array_shape, jnp.float32), -5.0, 5.0)
    return values.astype(jnp.bfloat16)


def layer_shuffle(key):
    layer_key = jax.random.fold_in(key, 21)

    def one_layer(layer):
        return jax.random.permutation(jax.random.fold_in(layer_key, layer), ADAPTER_COUNT).astype(jnp.int32)
    layers = jnp.arange(N_SECTION, dtype=jnp.int32)
    return jax.vmap(one_layer)(layers)


def draw_layer_page_slot(key, part):
    shuffled = layer_shuffle(key)
    layers = jnp.arange(N_SECTION, dtype=jnp.int32)
    return (shuffled + layers[:, None] * ADAPTER_COUNT).reshape(N_SECTION * ADAPTER_COUNT).astype(jnp.int32)


def draw_request_adapter(key, part):
    shuffled = layer_shuffle(key)
    inverse = jnp.argsort(shuffled, axis=1, stable=True).astype(jnp.int32)
    base_key = jax.random.fold_in(key, 31)
    array_shape = (N_SECTION, N_POOL, GROUP_REQUESTS)
    busy_section = jax.random.randint(jax.random.fold_in(base_key, 1), (), 0, N_SECTION, jnp.int32)
    busy_owner = jax.random.randint(jax.random.fold_in(base_key, 2), (N_SECTION,), 0, N_POOL, jnp.int32)
    group_owner = jax.random.randint(jax.random.fold_in(base_key, 3), (N_SECTION, N_POOL), 0, N_POOL, jnp.int32)
    within = jax.random.randint(jax.random.fold_in(base_key, 4), array_shape, 0, PAGES_DEV, jnp.int32)
    first_pick = jax.random.randint(jax.random.fold_in(base_key, 5), array_shape, 0, ADAPTER_COUNT, jnp.int32)
    second_pick = jax.random.randint(jax.random.fold_in(base_key, 6), array_shape, 0, ADAPTER_COUNT, jnp.int32)
    rotation = jax.random.randint(jax.random.fold_in(base_key, 7), (N_SECTION, 1, 1), 0, ADAPTER_COUNT, jnp.int32)
    coin_flip = jax.random.randint(jax.random.fold_in(base_key, 8), array_shape, 0, 2, jnp.int32)
    spread_slot = (jnp.minimum(first_pick, second_pick) + rotation) % ADAPTER_COUNT
    owner_slot = group_owner[:, :, None] * PAGES_DEV + within
    busy_slot = busy_owner[:, None, None] * PAGES_DEV + within
    is_busy = (jnp.arange(N_SECTION, dtype=jnp.int32) == busy_section)[:, None, None]
    slot_local = jnp.where(is_busy, busy_slot, jnp.where(coin_flip == 1, owner_slot, spread_slot)).astype(jnp.int32)
    adapters = jnp.take_along_axis(inverse, slot_local.reshape(N_SECTION, N_POOL * GROUP_REQUESTS), axis=1)
    return adapters.reshape(array_shape).astype(jnp.int32)


def set_ends(entries, key, low, high):
    longest = entries.shape.index(max(entries.shape))
    spots = []
    for shift in (0, 1):
        where = [jax.random.randint(jax.random.fold_in(key, axis), (), 0, length) for axis, length in enumerate(entries.shape)]
        where[longest] = (where[longest] + shift) % entries.shape[longest]
        spots.append(tuple(where))
    return entries.at[spots[0]].set(low).at[spots[1]].set(high)


def spiked(drawn, rng, source, target, shards_of, factor):
    owner, partner = [(jnp.arange(drawn.shape[axis_at]) // (drawn.shape[axis_at] // shards_of)).reshape([-1 if axis == axis_at else 1 for axis in range(drawn.ndim)]) for axis_at in (source, target)]
    chosen = jax.random.permutation(rng, shards_of)[partner]
    strong = (owner == chosen) | (owner == (partner + shards_of // 2) % shards_of)
    return jnp.where(strong, factor * drawn, drawn)


def block_levels(own_key, shape, pieces, smallest, top_value):
    factor_of = 1.0
    for dim, parts in pieces:
        heights = jax.random.uniform(jax.random.fold_in(jax.random.fold_in(own_key, 6), dim), (parts,), jnp.float32, smallest / len(pieces), top_value / len(pieces))
        factor_of = factor_of * jnp.repeat(jnp.exp(heights), shape[dim] // parts).reshape((-1,) + (1,) * (len(shape) - 1 - dim))
    return factor_of


def length_profile(amount, total, most, skew):
    weights = [(1 << 20) // math.isqrt(standing ** skew) + 1 for standing in range(2, amount + 1)]
    rest, counts = total - most - (amount - 1), [1] * (amount - 1)
    while rest > 0:
        free = [i for i in range(amount - 1) if counts[i] < most]
        whole, left = sum([weights[i] for i in free]), rest
        for i in free:
            addition = min(most - counts[i], max(1, left * weights[i] // whole), rest)
            counts[i] = counts[i] + addition
            rest = rest - addition
    return np.array([most] + counts)


def ragged_sizes(rng, amount, total, reach, skew):
    if amount == 2:
        one = jax.random.randint(rng, (), max(1, total - reach), min(reach, total - 1) + 1)
        return jnp.stack([one, total - one])
    tallies = jnp.asarray(length_profile(amount, total, reach, skew), jnp.int32)
    couples = (amount - 1) // 2
    donor, sink = tallies[1:1 + 2 * couples:2], tallies[2:2 + 2 * couples:2]
    margin = jnp.minimum(donor - 1, reach - sink)
    moved = jax.random.randint(jax.random.fold_in(rng, 1), (couples,), 0, 1 << 20) % (margin + 1)
    tallies = tallies.at[1:1 + 2 * couples:2].set(donor - moved).at[2:2 + 2 * couples:2].set(sink + moved)
    return tallies[jax.random.permutation(jax.random.fold_in(rng, 2), amount)]


def scatter_about(own_key, dims, width, bound, shards=(), kind=jnp.bfloat16):
    array = jax.random.normal(own_key, dims, jnp.float32) * width
    if len(shards) > 0:
        array = block_levels(own_key, dims, shards, -0.22, 0.18) * array
    return jnp.clip(array, min=-bound, max=bound).astype(kind)


def bell_draw_with(key, extent, deviation, reach, shards, heavy, kind=jnp.bfloat16):
    array = deviation * jax.random.normal(key, extent, jnp.float32)
    if shards:
        array = array * block_levels(key, extent, shards, -0.22, 0.18)
    return jnp.clip(spiked(array, jax.random.fold_in(key, 3), *heavy), -reach, reach).astype(kind)


def setup_inputs(seed: int = 0) -> dict:
    key_list = jax.random.split(jax.random.key(seed), 12)
    hidden = scatter_about(key_list[0], (N_SECTION, N_POOL, GROUP_REQUESTS * WINDOW_TOKENS, MODEL_WIDTH), 1.0, 6.0, ((0, 2), (1, 16), (3, 4)))
    queries = draw_queries(jax.random.fold_in(key_list[11], 71), 0)
    window_key_value = scatter_about(key_list[2], (N_SECTION, N_POOL, GROUP_REQUESTS, 2, KV_HEADS, WINDOW_TOKENS, HEAD_WIDTH), 2.0, 12.0, ((0, 2), (1, 16), (4, 4)))
    cached_key_value = scatter_about(key_list[3], (N_SECTION, N_POOL, CACHE_PAGES, 2, KV_HEADS, PAGE_TOK, HEAD_WIDTH), 2.0, 12.0, ((0, 2), (1, 16), (4, 4)))
    cached_length = jax.vmap(lambda own: ragged_sizes(own, GROUP_REQUESTS, GROUP_REQUESTS * MAX_PAGES * PAGE_TOK * 3 // 8, MAX_PAGES * PAGE_TOK, 2))(jax.random.split(key_list[4], N_SECTION * N_POOL)).reshape((N_SECTION, N_POOL, GROUP_REQUESTS)).astype(jnp.int32)
    request_page_table = set_ends(jax.random.randint(key_list[5], (N_SECTION, N_POOL, GROUP_REQUESTS, MAX_PAGES), 0, CACHE_PAGES), jax.random.fold_in(key_list[5], 1), 0, CACHE_PAGES - 1).astype(jnp.int32)
    request_adapter = draw_request_adapter(jax.random.fold_in(key_list[11], 71), 0)
    layer_page_slot = draw_layer_page_slot(jax.random.fold_in(key_list[11], 71), 0)
    wo = bell_draw_with(key_list[8], (N_SECTION, QUERY_HEADS * HEAD_WIDTH, MODEL_WIDTH), (QUERY_HEADS * HEAD_WIDTH) ** -0.5, 0.09375, ((0, 2), (1, 4)), (1, 2, 4, 2.0))
    adapter_down = scatter_about(key_list[9], (N_SECTION * ADAPTER_COUNT, ADAPTER_RANK, QUERY_HEADS * HEAD_WIDTH), (QUERY_HEADS * HEAD_WIDTH) ** -0.5, 0.0625, ((0, 32), (2, 4)))
    adapter_up = scatter_about(key_list[10], (N_SECTION * ADAPTER_COUNT, ADAPTER_RANK, MODEL_WIDTH), ADAPTER_RANK ** -0.5, 0.75, ((0, 32), (2, 4)))
    return dict(hidden=hidden, queries=queries, window_key_value=window_key_value, cached_key_value=cached_key_value, cached_length=cached_length, request_page_table=request_page_table, request_adapter=request_adapter, layer_page_slot=layer_page_slot, wo=wo, adapter_down=adapter_down, adapter_up=adapter_up)


def attend(queries, cache_pages, window_kv, lengths, page_rows):
    requests, window, head_count, head_size = queries.shape
    kv_heads = window_kv.shape[2]
    page_tok = cache_pages.shape[3]
    max_pages = page_rows.shape[1]
    cached = max_pages * page_tok
    picked = jnp.take(cache_pages, page_rows, axis=0)
    picked = jnp.transpose(picked, (0, 2, 3, 1, 4, 5)).reshape(requests, 2, kv_heads, cached, head_size)
    keys_all = jnp.concatenate([picked, window_kv], axis=3).astype(jnp.float32)
    grouped = queries.reshape(requests, window, kv_heads, head_count // kv_heads, head_size).astype(jnp.float32)
    scores = jnp.einsum("rwkgd,rktd->rkgwt", grouped, keys_all[:, 0], precision=lax.Precision.HIGHEST) * (head_size ** -0.5)
    position = jnp.arange(cached + window, dtype=jnp.int32)
    query_pos = jnp.arange(window, dtype=jnp.int32)
    in_cache = position[None, :] < lengths[:, None]
    in_window = (position[None, :] >= cached) & (position[None, :] - cached <= query_pos[:, None])
    allowed = in_cache[:, None, :] | in_window[None, :, :]
    scores = jnp.where(allowed[:, None, None, :, :], scores, -jnp.inf)
    largest = jnp.max(scores, axis=-1, keepdims=True)
    weights = jnp.exp(scores - largest)
    probs = (weights / jnp.sum(weights, axis=-1, keepdims=True)).astype(jnp.bfloat16)
    context = jnp.einsum("rkgwt,rktd->rwkgd", probs.astype(jnp.float32), keys_all[:, 1], precision=lax.Precision.HIGHEST)
    return context.reshape(requests, window, head_count * head_size).astype(jnp.bfloat16)


def reference(hidden, queries, window_key_value, cached_key_value, cached_length, request_page_table, request_adapter, layer_page_slot, wo, adapter_down, adapter_up):
    def one_group(group_id):
        section_index = group_id // N_POOL
        pool_index = group_id % N_POOL
        context = attend(queries[section_index, pool_index], cached_key_value[section_index, pool_index], window_key_value[section_index, pool_index], cached_length[section_index, pool_index], request_page_table[section_index, pool_index])
        flat_rows = context.reshape(GROUP_REQUESTS * WINDOW_TOKENS, QUERY_HEADS * HEAD_WIDTH)
        plain_output = jnp.dot(flat_rows, wo[section_index], preferred_element_type=jnp.float32)
        slot_indices = layer_page_slot[section_index * ADAPTER_COUNT + request_adapter[section_index, pool_index]].astype(jnp.int32)
        chosen_down = jnp.take(adapter_down, slot_indices, axis=0).astype(jnp.float32)
        chosen_up = jnp.take(adapter_up, slot_indices, axis=0).astype(jnp.float32)
        rank_hidden = jnp.einsum("rwh,rkh->rwk", context.astype(jnp.float32), chosen_down, precision=lax.Precision.HIGHEST).astype(jnp.bfloat16)
        adapter_delta = jnp.einsum("tol,tlh->toh", rank_hidden.astype(jnp.float32), chosen_up, precision=lax.Precision.HIGHEST).astype(jnp.bfloat16)
        adapter_delta = adapter_delta.reshape(GROUP_REQUESTS * WINDOW_TOKENS, MODEL_WIDTH).astype(jnp.float32)
        blended_output = hidden[section_index, pool_index].astype(jnp.float32) + plain_output + adapter_delta
        return blended_output.astype(jnp.bfloat16)

    results = lax.map(one_group, jnp.arange(N_SECTION * N_POOL, dtype=jnp.int32))
    results = results.reshape(N_SECTION, N_POOL, GROUP_REQUESTS * WINDOW_TOKENS, MODEL_WIDTH)
    return jnp.roll(results, 1, axis=0)
```

```python
import functools

import jax
import jax.numpy as jnp
from jax import lax
from jax.experimental import pallas as pl
from jax.experimental.pallas import tpu as pltpu
from jax.sharding import PartitionSpec as P

F32 = jnp.float32
BF16 = jnp.bfloat16
VMEM = pltpu.VMEM
NT = (((1,), (1,)), ((), ()))
TN = (((0,), (0,)), ((), ()))


def vspec():
    return pl.BlockSpec(memory_space=pltpu.VMEM)


def sspec():
    return pl.BlockSpec(memory_space=pltpu.SMEM)


def aspec():
    return pl.BlockSpec(memory_space=pl.ANY)


BUCKETS = (4, 8, 16)


def attend_kernel(
    len_ref, table_ref, q_ref, wkv_ref, cache_ref, heads_ref, flat_ref, slot, ctx32, sems
):
    requests = q_ref.shape[0]
    page = cache_ref.shape[3]
    scale = q_ref.shape[3] ** (-0.5)

    def bucket(r, fn):
        length = len_ref[r]
        low = 0
        for pages in BUCKETS:
            high = pages * page

            @pl.when((length > low) & (length <= high))
            def _():
                fn(pages)

            low = high

    def fetch(r, carry):
        def start(pages):
            for j in range(pages):
                pltpu.make_async_copy(
                    cache_ref.at[table_ref[r, j]], slot.at[r, j], sems.at[r]
                ).start()

        bucket(r, start)
        return carry

    lax.fori_loop(0, requests, fetch, 0)

    def one(r, carry):
        length = len_ref[r]
        zero = jnp.zeros(q_ref.shape[2:], BF16)
        query = jnp.concatenate(
            [
                jnp.concatenate([q_ref[r, 0], zero], axis=1),
                jnp.concatenate([zero, q_ref[r, 1]], axis=1),
            ],
            axis=0,
        )
        window_key = jnp.concatenate([wkv_ref[r, 0, 0], wkv_ref[r, 0, 1]], axis=1)
        window_value = jnp.concatenate([wkv_ref[r, 1, 0], wkv_ref[r, 1, 1]], axis=1)

        def work(pages):
            pltpu.make_async_copy(
                cache_ref.at[0:pages], slot.at[r, 0:pages], sems.at[r]
            ).wait()
            count = pages * page

            def side(kv, head):
                return slot[r, 0:pages, kv, head].reshape(count, 128)

            keys = jnp.concatenate([side(0, 0), side(0, 1)], axis=1)
            values = jnp.concatenate([side(1, 0), side(1, 1)], axis=1)
            s = lax.dot_general(keys, query, NT, preferred_element_type=F32) * scale
            position = lax.broadcasted_iota(jnp.int32, s.shape, 0)
            s = jnp.where(position < length, s, -1e30)
            sw = lax.dot_general(window_key, query, NT, preferred_element_type=F32) * scale
            row = lax.broadcasted_iota(jnp.int32, sw.shape, 0)
            token = lax.broadcasted_iota(jnp.int32, sw.shape, 1) % 8
            sw = jnp.where(row <= token, sw, -1e30)
            top = jnp.maximum(
                jnp.max(s, axis=0, keepdims=True), jnp.max(sw, axis=0, keepdims=True)
            )
            p = jnp.exp(s - top)
            pw = jnp.exp(sw - top)
            total = jnp.sum(p, axis=0, keepdims=True) + jnp.sum(pw, axis=0, keepdims=True)
            inverse = 1.0 / total
            p = (p * inverse).astype(BF16)
            pw = (pw * inverse).astype(BF16)
            out = lax.dot_general(p, values, TN, preferred_element_type=F32)
            out = out + lax.dot_general(pw, window_value, TN, preferred_element_type=F32)
            rows = pl.ds(pl.multiple_of(r * 8, 8), 8)
            ctx32[0:8, rows, :] = out[0:64, 0:128].reshape(8, 8, 128)
            ctx32[8:16, rows, :] = out[64:128, 128:256].reshape(8, 8, 128)

        bucket(r, work)
        return carry

    lax.fori_loop(0, requests, one, 0)
    for h in range(heads_ref.shape[0]):
        block = ctx32[h].astype(BF16)
        heads_ref[h] = block
        flat_ref[:, h * 128 : (h + 1) * 128] = block


def attend(queries, cache_pages, window_kv, lengths, page_rows):
    requests, window, head_count, head_size = queries.shape
    q = queries.transpose(0, 2, 1, 3).reshape(requests, 2, head_count // 2 * window, head_size)
    rows = requests * window
    return pl.pallas_call(
        attend_kernel,
        out_shape=(
            jax.ShapeDtypeStruct((head_count, rows, head_size), BF16),
            jax.ShapeDtypeStruct((rows, head_count * head_size), BF16),
        ),
        in_specs=[sspec(), sspec(), vspec(), vspec(), aspec()],
        out_specs=(vspec(), vspec()),
        scratch_shapes=[
            pltpu.VMEM((requests, 16) + cache_pages.shape[1:], BF16),
            pltpu.VMEM((head_count, rows, head_size), F32),
            pltpu.SemaphoreType.DMA((requests,)),
        ],
        compiler_params=pltpu.CompilerParams(vmem_limit_bytes=40 * 2**20),
        cost_estimate=pl.CostEstimate(
            flops=12 * 10**9, bytes_accessed=10 * 2**20, transcendentals=10**6
        ),
        name="attend",
    )(lengths, page_rows, q, window_kv, cache_pages)


def own_block(shape):
    row = lax.broadcasted_iota(jnp.int32, shape, 0) // 8
    col = lax.broadcasted_iota(jnp.int32, shape, 1) // 64
    return row == col


def down_kernel(slot_ref, ctx_ref, down_ref, z_ref):
    low = lax.broadcasted_iota(jnp.int32, (32, 128), 1) < 64
    keep = own_block((32, 256))

    def block(p, carry):
        parts = []
        for g in range(4):
            first = p * 16 + g * 4
            pages = jnp.concatenate([down_ref[slot_ref[first + a]] for a in range(4)], axis=0)
            rows = ctx_ref[p, g * 32 : (g + 1) * 32, :]
            wide = lax.dot_general(rows, pages, NT, preferred_element_type=F32)
            wide = jnp.where(keep, wide, 0.0)
            half = wide[:, 0:128] + wide[:, 128:256]
            parts.append(half + pltpu.roll(half, 64, 1))
        z_ref[p, 0:32, :] = jnp.where(low, parts[0], parts[2])
        z_ref[p, 32:64, :] = jnp.where(low, parts[1], parts[3])
        return carry

    lax.fori_loop(0, ctx_ref.shape[0], block, 0)


def up_kernel(slot_ref, z_ref, up_ref, out_ref):
    low = lax.broadcasted_iota(jnp.int32, (32, 128), 1) < 64
    keep = own_block((32, 256))

    def block(p, carry):
        parts = [None] * 4
        for half in range(2):
            x = z_ref[p, half * 32 : half * 32 + 32, :]
            turned = pltpu.roll(x, 64, 1)
            parts[half] = jnp.where(low, x, turned)
            parts[half + 2] = jnp.where(low, turned, x)
        for g in range(4):
            first = p * 16 + g * 4
            pages = jnp.concatenate([up_ref[slot_ref[first + a]] for a in range(4)], axis=0)
            twice = jnp.concatenate([parts[g], parts[g]], axis=1)
            rows = jnp.where(keep, twice, 0.0).astype(BF16)
            out = jnp.dot(rows, pages, preferred_element_type=F32)
            out_ref[p, g * 32 : (g + 1) * 32, :] = out.astype(BF16)
        return carry

    lax.fori_loop(0, z_ref.shape[0], block, 0)


def down_call(slots, ctx_all, down_all):
    n = ctx_all.shape[0]
    return pl.pallas_call(
        down_kernel,
        out_shape=jax.ShapeDtypeStruct((n, 64, 128), F32),
        in_specs=[sspec(), vspec(), vspec()],
        out_specs=vspec(),
        compiler_params=pltpu.CompilerParams(vmem_limit_bytes=16 * 2**20),
        cost_estimate=pl.CostEstimate(
            flops=4 * 10**9, bytes_accessed=3 * 2**20, transcendentals=0
        ),
        name="rank_down",
    )(slots, ctx_all, down_all)


def up_call(slots, z, up_all):
    n = z.shape[0]
    return pl.pallas_call(
        up_kernel,
        out_shape=jax.ShapeDtypeStruct((n, 128, 128), BF16),
        in_specs=[sspec(), vspec(), vspec()],
        out_specs=vspec(),
        compiler_params=pltpu.CompilerParams(vmem_limit_bytes=16 * 2**20),
        cost_estimate=pl.CostEstimate(
            flops=4 * 10**9, bytes_accessed=3 * 2**20, transcendentals=0
        ),
        name="rank_up",
    )(slots, z, up_all)


def spread_columns(pages):
    count, rank, width = pages.shape
    n = lax.axis_size("pool")
    x = pages.reshape(count * rank, n, width // n).transpose(1, 0, 2)
    x = lax.all_to_all(x, "pool", split_axis=0, concat_axis=0, tiled=True)
    return x.reshape(n * count, rank, width // n)


def per_device(
    hidden,
    queries,
    window_key_value,
    cached_key_value,
    cached_length,
    request_page_table,
    request_adapter,
    layer_page_slot,
    wo,
    adapter_down,
    adapter_up,
):
    section_count = lax.axis_size("section")
    section_index = lax.axis_index("section")
    adapters = layer_page_slot.shape[0] // section_count
    layer_start = section_index * adapters
    down_all = spread_columns(adapter_down)
    up_all = spread_columns(adapter_up)
    slots = (
        layer_page_slot[layer_start + request_adapter[section_index].reshape(-1)] - layer_start
    ).astype(jnp.int32)
    heads, flat = attend(
        queries[0, 0],
        cached_key_value[0, 0],
        window_key_value[0, 0],
        cached_length[0, 0],
        request_page_table[0, 0],
    )
    ctx_all = lax.all_to_all(heads, "pool", split_axis=0, concat_axis=0, tiled=True)
    partial_out = jnp.dot(flat, wo[0], preferred_element_type=F32)
    plain_output = lax.psum_scatter(partial_out, "tp", scatter_dimension=1, tiled=True)
    z = down_call(slots, ctx_all, down_all)
    z = lax.psum(z, ("tp", "pool"))
    z = z.astype(BF16).astype(F32)
    delta = up_call(slots, z, up_all)
    back = lax.all_to_all(delta, "pool", split_axis=0, concat_axis=0, tiled=True)
    rows, width = hidden.shape[2:]
    adapter_delta = back.transpose(1, 0, 2).reshape(rows, width).astype(F32)
    blended = (hidden[0, 0].astype(F32) + plain_output + adapter_delta).astype(BF16)
    handed = lax.ppermute(
        blended, "section", [(k, (k + 1) % section_count) for k in range(section_count)]
    )
    return handed[None, None]


def solution(mesh):
    return jax.shard_map(
        per_device,
        mesh=mesh,
        in_specs=(
            P("section", "pool", None, "tp"),
            P("section", "pool", None, None, "tp", None),
            P("section", "pool", None, None, "tp", None, None),
            P("section", "pool", None, None, "tp", None, None),
            P("section", "pool", None),
            P("section", "pool", None, None),
            P(),
            P(),
            P("section", "tp", None),
            P(("section", "pool"), None, "tp"),
            P(("section", "pool"), None, "tp"),
        ),
        out_specs=P("section", "pool", None, "tp"),
        check_vma=False,
    )
```

```python
import functools

import jax
import jax.numpy as jnp
from jax import lax
from jax.experimental import pallas as pl
from jax.experimental.pallas import tpu as pltpu
from jax.sharding import PartitionSpec as P

F32 = jnp.float32
BF16 = jnp.bfloat16
NT = (((1,), (1,)), ((), ()))
TN = (((0,), (0,)), ((), ()))
MESH = pl.DeviceIdType.MESH
SIDE = 4
POOL = SIDE * SIDE
SELF = 10
HEAD = 128
TILE = 512
BUFS = 3
BATCH = ((0, 4), (4, 9), (9, 16))


def own_block(shape):
    row = lax.broadcasted_iota(jnp.int32, shape, 0) // 8
    col = lax.broadcasted_iota(jnp.int32, shape, 1) // 64
    return row == col


def attend_one(r, len_ref, table_ref, q_ref, wkv_ref, cache_ref, ctx32):
    scale = HEAD ** (-0.5)
    pages = table_ref.shape[3]
    length = len_ref[0, 0, r]
    zero = jnp.zeros(q_ref.shape[2:], BF16)
    query = jnp.concatenate(
        [
            jnp.concatenate([q_ref[r, 0], zero], axis=1),
            jnp.concatenate([zero, q_ref[r, 1]], axis=1),
        ],
        axis=0,
    )
    window_key = jnp.concatenate([wkv_ref[r, 0, 0], wkv_ref[r, 0, 1]], axis=1)
    window_value = jnp.concatenate([wkv_ref[r, 1, 0], wkv_ref[r, 1, 1]], axis=1)

    def side(kv):
        return jnp.concatenate(
            [
                jnp.concatenate(
                    [
                        cache_ref[table_ref[0, 0, r, j], kv, 0],
                        cache_ref[table_ref[0, 0, r, j], kv, 1],
                    ],
                    axis=1,
                )
                for j in range(pages)
            ],
            axis=0,
        )

    s = lax.dot_general(side(0), query, NT, preferred_element_type=F32) * scale
    position = lax.broadcasted_iota(jnp.int32, s.shape, 0)
    s = jnp.where(position < length, s, -1e30)
    sw = lax.dot_general(window_key, query, NT, preferred_element_type=F32) * scale
    row = lax.broadcasted_iota(jnp.int32, sw.shape, 0)
    token = lax.broadcasted_iota(jnp.int32, sw.shape, 1) % 8
    sw = jnp.where(row <= token, sw, -1e30)
    top = jnp.maximum(jnp.max(s, axis=0, keepdims=True), jnp.max(sw, axis=0, keepdims=True))
    p = jnp.exp(s - top)
    pw = jnp.exp(sw - top)
    total = jnp.sum(p, axis=0, keepdims=True) + jnp.sum(pw, axis=0, keepdims=True)
    inverse = 1.0 / total
    p = (p * inverse).astype(BF16)
    pw = (pw * inverse).astype(BF16)
    out = lax.dot_general(p, side(1), TN, preferred_element_type=F32)
    out = out + lax.dot_general(pw, window_value, TN, preferred_element_type=F32)
    rows = pl.ds(pl.multiple_of(r * 8, 8), 8)
    ctx32[0:8, rows, :] = out[0:64, 0:128].reshape(8, 8, 128)
    ctx32[8:16, rows, :] = out[64:128, 128:256].reshape(8, 8, 128)


def kernel(
    len_ref,
    table_ref,
    adapter_ref,
    layer_ref,
    q_ref,
    wkv_hbm,
    cache_hbm,
    down_hbm,
    up_hbm,
    hidden_hbm,
    wo_hbm,
    out_ref,
    cache,
    wkv,
    hidden,
    down_stage,
    up_stage,
    down_all,
    up_all,
    ctx32,
    heads,
    flat,
    ctx_all,
    wbuf,
    far_send,
    far_recv,
    part,
    near_send,
    near_recv,
    own,
    z_send,
    z_recv,
    zt_send,
    zt_recv,
    z_own,
    z_all,
    delta_send,
    delta_recv,
    final,
    lsem,
    wsem,
    down_s,
    down_r,
    up_s,
    up_r,
    ctx_s,
    ctx_r,
    z_s,
    z_r,
    za_s,
    za_r,
    delta_s,
    delta_r,
    tp_s,
    tp_r,
    zt_s,
    zt_r,
    sec_s,
    sec_r,
):
    me = lax.axis_index("pool")
    x = lax.axis_index("tp")
    sec = lax.axis_index("section")
    mz = me // SIDE
    my = lax.rem(me, SIDE)
    adapters = layer_ref.shape[0] // 2
    start = sec * adapters

    def slot(p, r):
        return lax.rem(layer_ref[start + adapter_ref[sec, p, r]], adapters)

    def peer(k):
        dz = k // SIDE + 2
        dy = lax.rem(k, SIDE) + 2
        return lax.rem(mz + dz, SIDE) * SIDE + lax.rem(my + dy, SIDE)

    def origin(k):
        dz = 6 - k // SIDE
        dy = 6 - lax.rem(k, SIDE)
        return lax.rem(mz + dz, SIDE) * SIDE + lax.rem(my + dy, SIDE)

    def each(low, high, fn):
        def step(k, carry):
            fn(k)
            return carry

        if low < SELF < high:
            lax.fori_loop(low, SELF, step, 0)
            lax.fori_loop(SELF + 1, high, step, 0)
        else:
            lax.fori_loop(low + (low == SELF), high - (high == SELF + 1), step, 0)

    def pool_copy(src, dst, ssem, rsem, k, to):
        return pltpu.make_async_remote_copy(
            src_ref=src,
            dst_ref=dst,
            send_sem=ssem.at[k],
            recv_sem=rsem.at[k],
            device_id={"pool": to},
            device_id_type=MESH,
        )

    def columns(ref, j):
        return ref.at[:, :, pl.ds(pl.multiple_of(j * HEAD, HEAD), HEAD)]

    held = down_hbm.shape[0]

    def pages_of(ref, j):
        return ref.at[pl.ds(j * held, held)]

    def stage_copy(ref, stage, full, k, base):
        j = peer(k)
        return pltpu.make_async_copy(columns(ref, j), stage.at[j], lsem.at[base + k])

    def own_copy(ref, full, base):
        return pltpu.make_async_copy(columns(ref, me), pages_of(full, me), lsem.at[base + SELF])

    quarter = cache.shape[0] // 4

    def cache_copy(i):
        return pltpu.make_async_copy(
            cache_hbm.at[0, 0, i * quarter : (i + 1) * quarter],
            cache.at[i * quarter : (i + 1) * quarter],
            lsem.at[32 + i],
        )

    wkv_copy = pltpu.make_async_copy(wkv_hbm.at[0, 0], wkv, lsem.at[36])
    hidden_copy = pltpu.make_async_copy(hidden_hbm.at[0, 0], hidden, lsem.at[37])

    each(0, POOL, lambda k: stage_copy(down_hbm, down_stage, down_all, k, 0).start())
    own_copy(down_hbm, down_all, 0).start()
    wkv_copy.start()
    for i in range(4):
        cache_copy(i).start()

    barrier = pltpu.get_barrier_semaphore()

    def greet(k):
        pl.semaphore_signal(barrier, inc=1, device_id={"pool": peer(k)}, device_id_type=MESH)

    each(0, POOL, greet)
    for o in (1, 2, 3):
        pl.semaphore_signal(
            barrier, inc=1, device_id={"tp": lax.rem(x + o, SIDE)}, device_id_type=MESH
        )
    pl.semaphore_signal(barrier, inc=1, device_id={"section": 1 - sec}, device_id_type=MESH)
    pl.semaphore_wait(barrier, POOL - 1 + 3 + 1)

    def send_down(k):
        stage_copy(down_hbm, down_stage, down_all, k, 0).wait()
        pool_copy(down_stage.at[peer(k)], pages_of(down_all, me), down_s, down_r, k, peer(k)).start()

    each(0, POOL, send_down)
    own_copy(down_hbm, down_all, 0).wait()

    wkv_copy.wait()
    for i in range(4):
        cache_copy(i).wait()

    each(0, POOL, lambda k: stage_copy(up_hbm, up_stage, up_all, k, 16).start())
    own_copy(up_hbm, up_all, 16).start()
    hidden_copy.start()

    def wo_copy(i):
        target = lax.rem(x + (2, 1, 3, 0)[i // 4], SIDE)
        col = target * (SIDE * TILE) + (i % 4) * TILE
        return pltpu.make_async_copy(
            wo_hbm.at[0, :, pl.ds(pl.multiple_of(col, TILE), TILE)],
            wbuf.at[i % BUFS],
            wsem.at[i % BUFS],
        )

    for i in range(BUFS):
        wo_copy(i).start()

    def attend_step(r, carry):
        attend_one(r, len_ref, table_ref, q_ref, wkv, cache, ctx32)
        return carry

    lax.fori_loop(0, q_ref.shape[0], attend_step, 0)
    for h in range(POOL):
        block = ctx32[h].astype(BF16)
        heads[h] = block
        flat[:, h * HEAD : (h + 1) * HEAD] = block

    def send_ctx(k):
        pool_copy(heads.at[peer(k)], ctx_all.at[me], ctx_s, ctx_r, k, peer(k)).start()

    each(0, POOL, send_ctx)
    ctx_all[me] = heads[me]

    def send_up(k):
        stage_copy(up_hbm, up_stage, up_all, k, 16).wait()
        pool_copy(up_stage.at[peer(k)], pages_of(up_all, me), up_s, up_r, k, peer(k)).start()

    each(*BATCH[0], send_up)
    own_copy(up_hbm, up_all, 16).wait()

    def wo_tile(i):
        wo_copy(i).wait()
        value = jnp.dot(flat[...], wbuf[i % BUFS], preferred_element_type=F32)
        cols = slice((i % 4) * TILE, (i % 4 + 1) * TILE)
        group = i // 4
        if group == 0:
            far_send[:, cols] = value.astype(BF16)
        elif group == 3:
            own[:, cols] = value
        else:
            part[group - 1, :, cols] = value
        if i + BUFS < 16:
            wo_copy(i + BUFS).start()

    def tp_copy(src, dst, i, step):
        return pltpu.make_async_remote_copy(
            src_ref=src,
            dst_ref=dst,
            send_sem=tp_s.at[i],
            recv_sem=tp_r.at[i],
            device_id={"tp": lax.rem(x + SIDE + step, SIDE)},
            device_id_type=MESH,
        )

    def far_copy(i, step):
        return tp_copy(far_send.at[pl.ds(i * 64, 64)], far_recv.at[i], i, step)

    def near_copy(i, step):
        return tp_copy(near_send.at[i], near_recv.at[i], 2 + i, step)

    for i in range(4):
        wo_tile(i)
    far_copy(0, 1).start()
    far_copy(1, -1).start()
    for i in range(4, 12):
        wo_tile(i)
    far_copy(0, 1).wait_recv()
    far_copy(1, -1).wait_recv()
    near_send[0, 0:64] = (part[0, 0:64] + far_recv[0].astype(F32)).astype(BF16)
    near_send[0, 64:128] = part[0, 64:128].astype(BF16)
    near_send[1, 0:64] = part[1, 0:64].astype(BF16)
    near_send[1, 64:128] = (part[1, 64:128] + far_recv[1].astype(F32)).astype(BF16)
    near_copy(0, 1).start()
    near_copy(1, -1).start()

    def wait_ctx(k):
        s = origin(k)
        pool_copy(heads.at[s], ctx_all.at[s], ctx_s, ctx_r, k, s).wait_recv()

    def wait_down(k):
        s = origin(k)
        pool_copy(down_stage.at[s], pages_of(down_all, s), down_s, down_r, k, s).wait_recv()

    each(0, POOL, wait_down)
    each(0, POOL, wait_ctx)

    low = lax.broadcasted_iota(jnp.int32, (32, 128), 1) < 64
    keep = own_block((32, 256))

    def gathered(ref, p, g):
        return jnp.concatenate([ref[slot(p, g * 4 + a)] for a in range(4)], axis=0)

    def down_block(p, carry):
        pieces = []
        for g in range(4):
            pages = gathered(down_all, p, g)
            rows = ctx_all[p, g * 32 : (g + 1) * 32, :]
            wide = lax.dot_general(rows, pages, NT, preferred_element_type=F32)
            wide = jnp.where(keep, wide, 0.0)
            half = wide[:, 0:128] + wide[:, 128:256]
            pieces.append(half + pltpu.roll(half, 64, 1))
        z_send[p, 0:32, :] = jnp.where(low, pieces[0], pieces[2]).astype(BF16)
        z_send[p, 32:64, :] = jnp.where(low, pieces[1], pieces[3]).astype(BF16)
        return carry

    lax.fori_loop(0, POOL, down_block, 0)

    def send_z(k):
        pool_copy(z_send.at[peer(k)], z_recv.at[me], z_s, z_r, k, peer(k)).start()

    each(0, POOL, send_z)
    z_recv[me] = z_send[me]
    each(*BATCH[1], send_up)

    for i in range(12, 14):
        wo_tile(i)

    def wait_z(k):
        s = origin(k)
        pool_copy(z_send.at[s], z_recv.at[s], z_s, z_r, k, s).wait_recv()

    each(0, POOL, wait_z)
    total = z_recv[0].astype(F32)
    for p in range(1, POOL):
        total = total + z_recv[p].astype(F32)
    zt_send[...] = total.astype(BF16)

    def zt_copy(o):
        return pltpu.make_async_remote_copy(
            src_ref=zt_send,
            dst_ref=zt_recv.at[o - 1],
            send_sem=zt_s.at[o - 1],
            recv_sem=zt_r.at[o - 1],
            device_id={"tp": lax.rem(x + o, SIDE)},
            device_id_type=MESH,
        )

    for o in (2, 1, 3):
        zt_copy(o).start()
    for i in range(14, 16):
        wo_tile(i)
    for o in (1, 2, 3):
        zt_copy(o).wait_recv()
    total = zt_send[...].astype(F32)
    for o in range(3):
        total = total + zt_recv[o].astype(F32)
    z_own[...] = total.astype(BF16)

    def send_za(k):
        pool_copy(z_own, z_all.at[me], za_s, za_r, k, peer(k)).start()

    each(0, POOL, send_za)
    z_all[me] = z_own[...]
    each(*BATCH[2], send_up)

    hidden_copy.wait()
    near_copy(0, 1).wait_recv()
    near_copy(1, -1).wait_recv()
    own[...] = (
        own[...]
        + hidden[...].astype(F32)
        + near_recv[0].astype(F32)
        + near_recv[1].astype(F32)
    )

    def wait_za(k):
        pool_copy(z_own, z_all.at[origin(k)], za_s, za_r, k, origin(k)).wait_recv()

    def wait_up(k):
        s = origin(k)
        pool_copy(up_stage.at[s], pages_of(up_all, s), up_s, up_r, k, s).wait_recv()

    each(0, POOL, wait_za)
    each(0, POOL, wait_up)

    def up_block(p):
        pieces = [None] * 4
        for h in range(2):
            v = z_all[p, h * 32 : h * 32 + 32, :].astype(F32)
            turned = pltpu.roll(v, 64, 1)
            pieces[h] = jnp.where(low, v, turned)
            pieces[h + 2] = jnp.where(low, turned, v)
        for g in range(4):
            pages = gathered(up_all, p, g)
            twice = jnp.concatenate([pieces[g], pieces[g]], axis=1)
            rows = jnp.where(keep, twice, 0.0).astype(BF16)
            out = jnp.dot(rows, pages, preferred_element_type=F32)
            delta_send[p, g * 32 : (g + 1) * 32, :] = out.astype(BF16)

    def delta_copy(k, s, j):
        return pool_copy(delta_send.at[j], delta_recv.at[s], delta_s, delta_r, k, j)

    def up_and_send(k):
        up_block(peer(k))
        delta_copy(k, me, peer(k)).start()

    each(0, POOL, up_and_send)
    up_block(me)
    delta_recv[me] = delta_send[me]

    def wait_delta(k):
        s = origin(k)
        delta_copy(k, s, s).wait_recv()

    each(0, POOL, wait_delta)

    def hand_copy(h):
        rows = pl.ds(h * 64, 64)
        return pltpu.make_async_remote_copy(
            src_ref=final.at[rows],
            dst_ref=out_ref.at[rows],
            send_sem=sec_s.at[h],
            recv_sem=sec_r.at[h],
            device_id={"section": 1 - sec},
            device_id_type=MESH,
        )

    for h in range(2):
        rows = slice(h * 64, (h + 1) * 64)
        for j in range(POOL):
            cols = slice(j * HEAD, (j + 1) * HEAD)
            final[rows, cols] = (own[rows, cols] + delta_recv[j, rows].astype(F32)).astype(BF16)
        hand_copy(h).start()

    def drain(k):
        j = peer(k)
        pool_copy(down_stage.at[j], pages_of(down_all, me), down_s, down_r, k, j).wait_send()
        pool_copy(up_stage.at[j], pages_of(up_all, me), up_s, up_r, k, j).wait_send()
        pool_copy(heads.at[j], ctx_all.at[me], ctx_s, ctx_r, k, j).wait_send()
        pool_copy(z_send.at[j], z_recv.at[me], z_s, z_r, k, j).wait_send()
        pool_copy(z_own, z_all.at[me], za_s, za_r, k, j).wait_send()
        delta_copy(k, me, j).wait_send()

    each(0, POOL, drain)
    for o in (1, 2, 3):
        zt_copy(o).wait_send()
    far_copy(0, 1).wait_send()
    far_copy(1, -1).wait_send()
    near_copy(0, 1).wait_send()
    near_copy(1, -1).wait_send()
    for h in range(2):
        hand_copy(h).wait_send()
        hand_copy(h).wait_recv()


def per_device(
    hidden,
    queries,
    window_key_value,
    cached_key_value,
    cached_length,
    request_page_table,
    request_adapter,
    layer_page_slot,
    wo,
    adapter_down,
    adapter_up,
):
    requests, window, head_count, head_size = queries.shape[2:]
    rows = requests * window
    width = hidden.shape[3]
    q = queries[0, 0].transpose(0, 2, 1, 3)
    q = q.reshape(requests, 2, head_count // 2 * window, head_size)
    pages = adapter_down.shape[:2] + (HEAD,)
    smem = pl.BlockSpec(memory_space=pltpu.SMEM)
    vmem = pl.BlockSpec(memory_space=pltpu.VMEM)
    hbm = pl.BlockSpec(memory_space=pl.ANY)
    dma = pltpu.SemaphoreType.DMA
    handed = pl.pallas_call(
        kernel,
        out_shape=jax.ShapeDtypeStruct((rows, width), BF16),
        in_specs=[smem, smem, smem, smem, vmem, hbm, hbm, hbm, hbm, hbm, hbm],
        out_specs=vmem,
        scratch_shapes=[
            pltpu.VMEM(cached_key_value.shape[2:], BF16),
            pltpu.VMEM(window_key_value.shape[2:], BF16),
            pltpu.VMEM((rows, width), BF16),
            pltpu.VMEM((POOL,) + pages, BF16),
            pltpu.VMEM((POOL,) + pages, BF16),
            pltpu.VMEM((POOL * pages[0],) + pages[1:], BF16),
            pltpu.VMEM((POOL * pages[0],) + pages[1:], BF16),
            pltpu.VMEM((POOL, rows, HEAD), F32),
            pltpu.VMEM((POOL, rows, HEAD), BF16),
            pltpu.VMEM((rows, width), BF16),
            pltpu.VMEM((POOL, rows, HEAD), BF16),
            pltpu.VMEM((BUFS, width, TILE), BF16),
            pltpu.VMEM((rows, width), BF16),
            pltpu.VMEM((2, 64, width), BF16),
            pltpu.VMEM((2, rows, width), F32),
            pltpu.VMEM((2, rows, width), BF16),
            pltpu.VMEM((2, rows, width), BF16),
            pltpu.VMEM((rows, width), F32),
            pltpu.VMEM((POOL, 64, HEAD), BF16),
            pltpu.VMEM((POOL, 64, HEAD), BF16),
            pltpu.VMEM((64, HEAD), BF16),
            pltpu.VMEM((3, 64, HEAD), BF16),
            pltpu.VMEM((64, HEAD), BF16),
            pltpu.VMEM((POOL, 64, HEAD), BF16),
            pltpu.VMEM((POOL, rows, HEAD), BF16),
            pltpu.VMEM((POOL, rows, HEAD), BF16),
            pltpu.VMEM((rows, width), BF16),
            dma((40,)),
            dma((BUFS,)),
            dma((POOL,)),
            dma((POOL,)),
            dma((POOL,)),
            dma((POOL,)),
            dma((POOL,)),
            dma((POOL,)),
            dma((POOL,)),
            dma((POOL,)),
            dma((POOL,)),
            dma((POOL,)),
            dma((POOL,)),
            dma((POOL,)),
            dma((4,)),
            dma((4,)),
            dma((3,)),
            dma((3,)),
            dma((2,)),
            dma((2,)),
        ],
        compiler_params=pltpu.CompilerParams(
            collective_id=0, has_side_effects=True, vmem_limit_bytes=60 * 2**20
        ),
        name="relay_layer",
    )(
        cached_length,
        request_page_table,
        request_adapter,
        layer_page_slot,
        q,
        window_key_value,
        cached_key_value,
        adapter_down,
        adapter_up,
        hidden,
        wo,
    )
    return handed[None, None]


def solution(mesh):
    return jax.shard_map(
        per_device,
        mesh=mesh,
        in_specs=(
            P("section", "pool", None, "tp"),
            P("section", "pool", None, None, "tp", None),
            P("section", "pool", None, None, "tp", None, None),
            P("section", "pool", None, None, "tp", None, None),
            P("section", "pool", None),
            P("section", "pool", None, None),
            P(),
            P(),
            P("section", "tp", None),
            P(("section", "pool"), None, "tp"),
            P(("section", "pool"), None, "tp"),
        ),
        out_specs=P("section", "pool", None, "tp"),
        check_vma=False,
    )
```

```python
import functools

import jax
import jax.numpy as jnp
from jax import lax
from jax.experimental import pallas as pl
from jax.experimental.pallas import tpu as pltpu
from jax.sharding import PartitionSpec as P

F32 = jnp.float32
BF16 = jnp.bfloat16
NT = (((1,), (1,)), ((), ()))
TN = (((0,), (0,)), ((), ()))
MESH = pl.DeviceIdType.MESH
SIDE = 4
POOL = SIDE * SIDE
HEAD = 128
TILE = 512
BUFS = 3
OFFSETS = (
    (2, 2), (1, 1), (3, 3), (1, 3), (3, 1),
    (2, 1), (2, 3), (0, 2), (1, 0), (3, 0),
    (1, 2), (3, 2), (2, 0), (0, 1), (0, 3),
)
EVEN = tuple(dz + SIDE * ((dy - dz) % SIDE) for dz, dy in OFFSETS)
BATCH = (EVEN[:7], EVEN[7:11], EVEN[11:])


def own_block(shape):
    row = lax.broadcasted_iota(jnp.int32, shape, 0) // 8
    col = lax.broadcasted_iota(jnp.int32, shape, 1) // 64
    return row == col


def attend_one(r, swap, len_ref, table_ref, q_ref, wkv_ref, cache_ref, ctx32):
    scale = HEAD ** (-0.5)
    pages = table_ref.shape[3]
    length = len_ref[0, 0, r]
    by_head = jnp.dot(swap, q_ref[r].reshape(128, HEAD), preferred_element_type=F32).astype(BF16)
    zero = jnp.zeros((64, HEAD), BF16)
    query = jnp.concatenate(
        [
            jnp.concatenate([by_head[0:64], zero], axis=1),
            jnp.concatenate([zero, by_head[64:128]], axis=1),
        ],
        axis=0,
    )
    window_key = jnp.concatenate([wkv_ref[r, 0, 0], wkv_ref[r, 0, 1]], axis=1)
    window_value = jnp.concatenate([wkv_ref[r, 1, 0], wkv_ref[r, 1, 1]], axis=1)

    def side(kv):
        return jnp.concatenate(
            [
                jnp.concatenate(
                    [
                        cache_ref[table_ref[0, 0, r, j], kv, 0],
                        cache_ref[table_ref[0, 0, r, j], kv, 1],
                    ],
                    axis=1,
                )
                for j in range(pages)
            ],
            axis=0,
        )

    s = lax.dot_general(side(0), query, NT, preferred_element_type=F32) * scale
    position = lax.broadcasted_iota(jnp.int32, s.shape, 0)
    s = jnp.where(position < length, s, -1e30)
    sw = lax.dot_general(window_key, query, NT, preferred_element_type=F32) * scale
    row = lax.broadcasted_iota(jnp.int32, sw.shape, 0)
    token = lax.broadcasted_iota(jnp.int32, sw.shape, 1) % 8
    sw = jnp.where(row <= token, sw, -1e30)
    top = jnp.maximum(jnp.max(s, axis=0, keepdims=True), jnp.max(sw, axis=0, keepdims=True))
    p = jnp.exp(s - top)
    pw = jnp.exp(sw - top)
    total = jnp.sum(p, axis=0, keepdims=True) + jnp.sum(pw, axis=0, keepdims=True)
    inverse = 1.0 / total
    p = (p * inverse).astype(BF16)
    pw = (pw * inverse).astype(BF16)
    out = lax.dot_general(p, side(1), TN, preferred_element_type=F32)
    out = out + lax.dot_general(pw, window_value, TN, preferred_element_type=F32)
    rows = pl.ds(pl.multiple_of(r * 8, 8), 8)
    ctx32[0:8, rows, :] = out[0:64, 0:128].reshape(8, 8, 128)
    ctx32[8:16, rows, :] = out[64:128, 128:256].reshape(8, 8, 128)


def kernel(
    len_ref,
    table_ref,
    adapter_ref,
    layer_ref,
    q_hbm,
    wkv_hbm,
    cache_hbm,
    down_hbm,
    up_hbm,
    hidden_hbm,
    wo_hbm,
    out_ref,
    cache,
    q_ref,
    wkv,
    hidden,
    down_stage,
    up_stage,
    down_all,
    up_all,
    ctx32,
    heads,
    flat,
    ctx_all,
    wbuf,
    far_send,
    far_recv,
    part,
    near_send,
    near_recv,
    own,
    z_send,
    zx_recv,
    zq_send,
    zq_recv,
    z_own,
    zq_all,
    z_all,
    delta_send,
    delta_recv,
    final,
    lsem,
    wsem,
    down_s,
    down_r,
    up_s,
    up_r,
    ctx_s,
    ctx_r,
    z_s,
    z_r,
    za_s,
    za_r,
    delta_s,
    delta_r,
    tp_s,
    tp_r,
    zx_s,
    zx_r,
    zt_s,
    zt_r,
    sec_s,
    sec_r,
):
    me = lax.axis_index("pool")
    x = lax.axis_index("tp")
    sec = lax.axis_index("section")
    mz = me // SIDE
    my = lax.rem(me, SIDE)
    adapters = layer_ref.shape[0] // 2
    start = sec * adapters

    def slot(p, r):
        return lax.rem(layer_ref[start + adapter_ref[sec, p, r]], adapters)

    def peer(k):
        dz = lax.rem(k, SIDE)
        dy = dz + k // SIDE
        return lax.rem(mz + dz, SIDE) * SIDE + lax.rem(my + dy, SIDE)

    def origin(k):
        dz = SIDE - lax.rem(k, SIDE)
        dy = dz + SIDE - k // SIDE
        return lax.rem(mz + dz, SIDE) * SIDE + lax.rem(my + dy, SIDE)

    def each(low, high, fn):
        def step(k, carry):
            fn(k)
            return carry

        lax.fori_loop(low, high, step, 0)

    def pool_copy(src, dst, ssem, rsem, k, to):
        return pltpu.make_async_remote_copy(
            src_ref=src,
            dst_ref=dst,
            send_sem=ssem.at[k],
            recv_sem=rsem.at[k],
            device_id={"pool": to},
            device_id_type=MESH,
        )

    def columns(ref, j):
        return ref.at[:, :, pl.ds(pl.multiple_of(j * HEAD, HEAD), HEAD)]

    held = down_hbm.shape[0]

    def pages_of(ref, j):
        return ref.at[pl.ds(j * held, held)]

    def stage_copy(ref, stage, full, k, base):
        j = peer(k)
        return pltpu.make_async_copy(columns(ref, j), stage.at[j], lsem.at[base + k])

    def own_copy(ref, full, base):
        return pltpu.make_async_copy(columns(ref, me), pages_of(full, me), lsem.at[base])

    quarter = cache.shape[0] // 4

    def cache_copy(i):
        return pltpu.make_async_copy(
            cache_hbm.at[0, 0, i * quarter : (i + 1) * quarter],
            cache.at[i * quarter : (i + 1) * quarter],
            lsem.at[32 + i],
        )

    wkv_copy = pltpu.make_async_copy(wkv_hbm.at[0, 0], wkv, lsem.at[36])
    query_copy = pltpu.make_async_copy(q_hbm.at[0, 0], q_ref, lsem.at[38])
    hidden_copy = pltpu.make_async_copy(hidden_hbm.at[0, 0], hidden, lsem.at[37])

    for k in EVEN:
        stage_copy(down_hbm, down_stage, down_all, k, 0).start()
    own_copy(down_hbm, down_all, 0).start()
    query_copy.start()
    wkv_copy.start()

    barrier = pltpu.get_barrier_semaphore()

    def greet(k):
        pl.semaphore_signal(barrier, inc=1, device_id={"pool": peer(k)}, device_id_type=MESH)

    each(1, POOL, greet)
    for o in (1, 2, 3):
        pl.semaphore_signal(
            barrier, inc=1, device_id={"tp": lax.rem(x + o, SIDE)}, device_id_type=MESH
        )
    pl.semaphore_signal(barrier, inc=1, device_id={"section": 1 - sec}, device_id_type=MESH)
    pl.semaphore_wait(barrier, POOL - 1 + 3 + 1)
    for i in range(4):
        cache_copy(i).start()

    def send_down(k):
        stage_copy(down_hbm, down_stage, down_all, k, 0).wait()
        pool_copy(down_stage.at[peer(k)], pages_of(down_all, me), down_s, down_r, k, peer(k)).start()

    for k in EVEN:
        send_down(k)
    own_copy(down_hbm, down_all, 0).wait()

    query_copy.wait()
    wkv_copy.wait()
    for i in range(4):
        cache_copy(i).wait()

    for k in EVEN:
        stage_copy(up_hbm, up_stage, up_all, k, 16).start()
    own_copy(up_hbm, up_all, 16).start()
    hidden_copy.start()

    def wo_copy(i):
        target = lax.rem(x + (2, 1, 3, 0)[i // 4], SIDE)
        col = target * (SIDE * TILE) + (i % 4) * TILE
        return pltpu.make_async_copy(
            wo_hbm.at[0, :, pl.ds(pl.multiple_of(col, TILE), TILE)],
            wbuf.at[i % BUFS],
            wsem.at[i % BUFS],
        )

    for i in range(BUFS):
        wo_copy(i).start()

    to = lax.broadcasted_iota(jnp.int32, (128, 128), 0)
    source = lax.broadcasted_iota(jnp.int32, (128, 128), 1)
    swap = jnp.where(source == (to % 8) * 16 + to // 8, 1.0, 0.0).astype(BF16)

    def attend_step(r, carry):
        attend_one(r, swap, len_ref, table_ref, q_ref, wkv, cache, ctx32)
        return carry

    lax.fori_loop(0, q_ref.shape[0], attend_step, 0)
    for h in range(POOL):
        block = ctx32[h].astype(BF16)
        heads[h] = block
        flat[:, h * HEAD : (h + 1) * HEAD] = block

    def send_ctx(k):
        pool_copy(heads.at[peer(k)], ctx_all.at[me], ctx_s, ctx_r, k, peer(k)).start()

    for k in EVEN:
        send_ctx(k)
    ctx_all[me] = heads[me]

    def send_up(k):
        stage_copy(up_hbm, up_stage, up_all, k, 16).wait()
        pool_copy(up_stage.at[peer(k)], pages_of(up_all, me), up_s, up_r, k, peer(k)).start()

    for k in BATCH[0]:
        send_up(k)
    own_copy(up_hbm, up_all, 16).wait()

    def wo_tile(i):
        wo_copy(i).wait()
        value = jnp.dot(flat[...], wbuf[i % BUFS], preferred_element_type=F32)
        cols = slice((i % 4) * TILE, (i % 4 + 1) * TILE)
        group = i // 4
        if group == 0:
            far_send[:, cols] = value.astype(BF16)
        elif group == 3:
            own[:, cols] = value
        else:
            part[group - 1, :, cols] = value
        if i + BUFS < 16:
            wo_copy(i + BUFS).start()

    def tp_copy(src, dst, i, step):
        return pltpu.make_async_remote_copy(
            src_ref=src,
            dst_ref=dst,
            send_sem=tp_s.at[i],
            recv_sem=tp_r.at[i],
            device_id={"tp": lax.rem(x + SIDE + step, SIDE)},
            device_id_type=MESH,
        )

    def far_copy(i, step):
        return tp_copy(far_send.at[pl.ds(i * 64, 64)], far_recv.at[i], i, step)

    def near_copy(i, half):
        rows = pl.ds(half * 64, 64)
        src, dst = near_send.at[i, rows], near_recv.at[i, rows]
        return tp_copy(src, dst, 2 + 2 * i + half, 1 - 2 * i)

    for i in range(4):
        wo_tile(i)
    far_copy(0, 1).start()
    far_copy(1, -1).start()
    for i in range(4, 12):
        wo_tile(i)
    near_send[0, 64:128] = part[0, 64:128].astype(BF16)
    near_send[1, 0:64] = part[1, 0:64].astype(BF16)
    near_copy(0, 1).start()
    near_copy(1, 0).start()
    far_copy(0, 1).wait_recv()
    far_copy(1, -1).wait_recv()
    near_send[0, 0:64] = (part[0, 0:64] + far_recv[0].astype(F32)).astype(BF16)
    near_send[1, 64:128] = (part[1, 64:128] + far_recv[1].astype(F32)).astype(BF16)

    def wait_ctx(k):
        s = origin(k)
        pool_copy(heads.at[s], ctx_all.at[s], ctx_s, ctx_r, k, s).wait_recv()

    def wait_down(k):
        s = origin(k)
        pool_copy(down_stage.at[s], pages_of(down_all, s), down_s, down_r, k, s).wait_recv()

    each(1, POOL, wait_down)
    each(1, POOL, wait_ctx)

    low = lax.broadcasted_iota(jnp.int32, (32, 128), 1) < 64
    keep = own_block((32, 256))

    def gathered(ref, p, g):
        return jnp.concatenate([ref[slot(p, g * 4 + a)] for a in range(4)], axis=0)

    def down_block(p, carry):
        pieces = []
        for g in range(4):
            pages = gathered(down_all, p, g)
            rows = ctx_all[p, g * 32 : (g + 1) * 32, :]
            wide = lax.dot_general(rows, pages, NT, preferred_element_type=F32)
            wide = jnp.where(keep, wide, 0.0)
            half = wide[:, 0:128] + wide[:, 128:256]
            pieces.append(half + pltpu.roll(half, 64, 1))
        z_send[p, 0:32, :] = jnp.where(low, pieces[0], pieces[2]).astype(BF16)
        z_send[p, 32:64, :] = jnp.where(low, pieces[1], pieces[3]).astype(BF16)
        return carry

    lax.fori_loop(0, POOL, down_block, 0)

    def quarter_rows(ref, o):
        return ref.at[:, pl.ds(pl.multiple_of(lax.rem(x + o, SIDE) * 16, 16), 16), :]

    def line_copy(src, dst, ssem, rsem, o):
        return pltpu.make_async_remote_copy(
            src_ref=src,
            dst_ref=dst,
            send_sem=ssem.at[o - 1],
            recv_sem=rsem.at[o - 1],
            device_id={"tp": lax.rem(x + o, SIDE)},
            device_id_type=MESH,
        )

    def part_copy(o):
        return line_copy(quarter_rows(z_send, o), zx_recv.at[o - 1], zx_s, zx_r, o)

    for o in (2, 1, 3):
        part_copy(o).start()
    near_copy(0, 0).start()
    near_copy(1, 1).start()
    for i in range(12, 14):
        wo_tile(i)
    for o in (1, 2, 3):
        part_copy(o).wait_recv()
    mine = pl.ds(pl.multiple_of(x * 16, 16), 16)
    total = z_send[:, mine, :].astype(F32)
    for o in range(3):
        total = total + zx_recv[o].astype(F32)
    zq_send[...] = total.astype(BF16)

    def send_z(k):
        pool_copy(zq_send.at[peer(k)], zq_recv.at[me], z_s, z_r, k, peer(k)).start()

    for k in EVEN:
        send_z(k)
    zq_recv[me] = zq_send[me]
    for k in BATCH[1]:
        send_up(k)
    wo_tile(14)

    def wait_z(k):
        s = origin(k)
        pool_copy(zq_send.at[s], zq_recv.at[s], z_s, z_r, k, s).wait_recv()

    each(1, POOL, wait_z)
    total = zq_recv[0].astype(F32)
    for p in range(1, POOL):
        total = total + zq_recv[p].astype(F32)
    z_own[...] = total.astype(BF16)

    def send_za(k):
        pool_copy(z_own, zq_all.at[me], za_s, za_r, k, peer(k)).start()

    for k in EVEN:
        send_za(k)
    zq_all[me] = z_own[...]
    for k in BATCH[2]:
        send_up(k)
    wo_tile(15)

    def wait_za(k):
        pool_copy(z_own, zq_all.at[origin(k)], za_s, za_r, k, origin(k)).wait_recv()

    each(1, POOL, wait_za)

    def whole_copy(o):
        rows = z_all.at[:, mine, :]
        return line_copy(zq_all, rows, zt_s, zt_r, o)

    def whole_wait(o):
        rows = quarter_rows(z_all, SIDE - o)
        line_copy(zq_all, rows, zt_s, zt_r, o).wait_recv()

    for o in (2, 1, 3):
        whole_copy(o).start()
    z_all[:, mine, :] = zq_all[...]

    hidden_copy.wait()
    for i in range(2):
        for half in range(2):
            near_copy(i, half).wait_recv()
    own[...] = (
        own[...]
        + hidden[...].astype(F32)
        + near_recv[0].astype(F32)
        + near_recv[1].astype(F32)
    )

    def wait_up(k):
        s = origin(k)
        pool_copy(up_stage.at[s], pages_of(up_all, s), up_s, up_r, k, s).wait_recv()

    for o in (1, 2, 3):
        whole_wait(o)
    each(1, POOL, wait_up)

    def up_block(p):
        pieces = [None] * 4
        for h in range(2):
            v = z_all[p, h * 32 : h * 32 + 32, :].astype(F32)
            turned = pltpu.roll(v, 64, 1)
            pieces[h] = jnp.where(low, v, turned)
            pieces[h + 2] = jnp.where(low, turned, v)
        for g in range(4):
            pages = gathered(up_all, p, g)
            twice = jnp.concatenate([pieces[g], pieces[g]], axis=1)
            rows = jnp.where(keep, twice, 0.0).astype(BF16)
            out = jnp.dot(rows, pages, preferred_element_type=F32)
            delta_send[p, g * 32 : (g + 1) * 32, :] = out.astype(BF16)

    def delta_copy(k, s, j):
        return pool_copy(delta_send.at[j], delta_recv.at[s], delta_s, delta_r, k, j)

    def up_and_send(k):
        up_block(peer(k))
        delta_copy(k, me, peer(k)).start()

    each(1, POOL, up_and_send)
    up_block(me)
    delta_recv[me] = delta_send[me]

    def wait_delta(k):
        s = origin(k)
        delta_copy(k, s, s).wait_recv()

    def hand_copy(j):
        return pltpu.make_async_remote_copy(
            src_ref=final.at[j],
            dst_ref=out_ref.at[:, pl.ds(pl.multiple_of(j * HEAD, HEAD), HEAD)],
            send_sem=sec_s.at[j],
            recv_sem=sec_r.at[j],
            device_id={"section": 1 - sec},
            device_id_type=MESH,
        )

    def finish(j):
        value = own[:, pl.ds(pl.multiple_of(j * HEAD, HEAD), HEAD)]
        final[j] = (value + delta_recv[j].astype(F32)).astype(BF16)
        hand_copy(j).start()

    finish(me)

    def take(k):
        wait_delta(k)
        finish(origin(k))

    each(1, POOL, take)

    def drain(k):
        j = peer(k)
        pool_copy(down_stage.at[j], pages_of(down_all, me), down_s, down_r, k, j).wait_send()
        pool_copy(up_stage.at[j], pages_of(up_all, me), up_s, up_r, k, j).wait_send()
        pool_copy(heads.at[j], ctx_all.at[me], ctx_s, ctx_r, k, j).wait_send()
        pool_copy(zq_send.at[j], zq_recv.at[me], z_s, z_r, k, j).wait_send()
        pool_copy(z_own, zq_all.at[me], za_s, za_r, k, j).wait_send()
        delta_copy(k, me, j).wait_send()

    each(1, POOL, drain)
    for o in (1, 2, 3):
        part_copy(o).wait_send()
        whole_copy(o).wait_send()
    far_copy(0, 1).wait_send()
    far_copy(1, -1).wait_send()
    for i in range(2):
        for half in range(2):
            near_copy(i, half).wait_send()

    def handed(j):
        hand_copy(j).wait_send()
        hand_copy(j).wait_recv()

    each(0, POOL, handed)


def per_device(
    hidden,
    queries,
    window_key_value,
    cached_key_value,
    cached_length,
    request_page_table,
    request_adapter,
    layer_page_slot,
    wo,
    adapter_down,
    adapter_up,
):
    rows = queries.shape[2] * queries.shape[3]
    width = hidden.shape[3]
    pages = adapter_down.shape[:2] + (HEAD,)
    smem = pl.BlockSpec(memory_space=pltpu.SMEM)
    vmem = pl.BlockSpec(memory_space=pltpu.VMEM)
    hbm = pl.BlockSpec(memory_space=pl.ANY)
    dma = pltpu.SemaphoreType.DMA
    handed = pl.pallas_call(
        kernel,
        out_shape=jax.ShapeDtypeStruct((rows, width), BF16),
        in_specs=[smem, smem, smem, smem, hbm, hbm, hbm, hbm, hbm, hbm, hbm],
        out_specs=vmem,
        scratch_shapes=[
            pltpu.VMEM(cached_key_value.shape[2:], BF16),
            pltpu.VMEM(queries.shape[2:], BF16),
            pltpu.VMEM(window_key_value.shape[2:], BF16),
            pltpu.VMEM((rows, width), BF16),
            pltpu.VMEM((POOL,) + pages, BF16),
            pltpu.VMEM((POOL,) + pages, BF16),
            pltpu.VMEM((POOL * pages[0],) + pages[1:], BF16),
            pltpu.VMEM((POOL * pages[0],) + pages[1:], BF16),
            pltpu.VMEM((POOL, rows, HEAD), F32),
            pltpu.VMEM((POOL, rows, HEAD), BF16),
            pltpu.VMEM((rows, width), BF16),
            pltpu.VMEM((POOL, rows, HEAD), BF16),
            pltpu.VMEM((BUFS, width, TILE), BF16),
            pltpu.VMEM((rows, width), BF16),
            pltpu.VMEM((2, 64, width), BF16),
            pltpu.VMEM((2, rows, width), F32),
            pltpu.VMEM((2, rows, width), BF16),
            pltpu.VMEM((2, rows, width), BF16),
            pltpu.VMEM((rows, width), F32),
            pltpu.VMEM((POOL, 64, HEAD), BF16),
            pltpu.VMEM((3, POOL, 16, HEAD), BF16),
            pltpu.VMEM((POOL, 16, HEAD), BF16),
            pltpu.VMEM((POOL, 16, HEAD), BF16),
            pltpu.VMEM((16, HEAD), BF16),
            pltpu.VMEM((POOL, 16, HEAD), BF16),
            pltpu.VMEM((POOL, 64, HEAD), BF16),
            pltpu.VMEM((POOL, rows, HEAD), BF16),
            pltpu.VMEM((POOL, rows, HEAD), BF16),
            pltpu.VMEM((POOL, rows, HEAD), BF16),
            dma((40,)),
            dma((BUFS,)),
            dma((POOL,)),
            dma((POOL,)),
            dma((POOL,)),
            dma((POOL,)),
            dma((POOL,)),
            dma((POOL,)),
            dma((POOL,)),
            dma((POOL,)),
            dma((POOL,)),
            dma((POOL,)),
            dma((POOL,)),
            dma((POOL,)),
            dma((6,)),
            dma((6,)),
            dma((3,)),
            dma((3,)),
            dma((3,)),
            dma((3,)),
            dma((POOL,)),
            dma((POOL,)),
        ],
        compiler_params=pltpu.CompilerParams(
            collective_id=0, has_side_effects=True, vmem_limit_bytes=60 * 2**20
        ),
        name="relay_layer",
    )(
        cached_length,
        request_page_table,
        request_adapter,
        layer_page_slot,
        queries,
        window_key_value,
        cached_key_value,
        adapter_down,
        adapter_up,
        hidden,
        wo,
    )
    return handed[None, None]


def solution(mesh):
    return jax.shard_map(
        per_device,
        mesh=mesh,
        in_specs=(
            P("section", "pool", None, "tp"),
            P("section", "pool", None, None, "tp", None),
            P("section", "pool", None, None, "tp", None, None),
            P("section", "pool", None, None, "tp", None, None),
            P("section", "pool", None),
            P("section", "pool", None, None),
            P(),
            P(),
            P("section", "tp", None),
            P(("section", "pool"), None, "tp"),
            P(("section", "pool"), None, "tp"),
        ),
        out_specs=P("section", "pool", None, "tp"),
        check_vma=False,
    )
```

```python
import functools

import jax
import jax.numpy as jnp
from jax import lax
from jax.experimental import pallas as pl
from jax.experimental.pallas import tpu as pltpu
from jax.sharding import PartitionSpec as P

F32 = jnp.float32
BF16 = jnp.bfloat16
NT = (((1,), (1,)), ((), ()))
MESH = pl.DeviceIdType.MESH
SIDE = 4
POOL = SIDE * SIDE
HEAD = 128
TILE = 512
BUFS = 3
OFFSETS = (
    (2, 2), (1, 1), (3, 3), (1, 3), (3, 1),
    (2, 1), (2, 3), (0, 2), (1, 0), (3, 0),
    (1, 2), (3, 2), (2, 0), (0, 1), (0, 3),
)
EVEN = tuple(dz + SIDE * ((dy - dz) % SIDE) for dz, dy in OFFSETS)
BATCH = (EVEN[:5], EVEN[5:], (), ())
ORDER = (2, 1, 3, 0)


def own_block(shape):
    row = lax.broadcasted_iota(jnp.int32, shape, 0) // 8
    col = lax.broadcasted_iota(jnp.int32, shape, 1) // 64
    return row == col


def attend_one(r, swap, len_ref, table_ref, q_ref, wkv_ref, cache_ref, ctx32):
    scale = HEAD ** (-0.5)
    pages = table_ref.shape[3]
    length = len_ref[0, 0, r]
    by_head = jnp.dot(swap, q_ref[r].reshape(128, HEAD), preferred_element_type=F32).astype(BF16)
    zero = jnp.zeros((64, HEAD), BF16)
    query = jnp.concatenate(
        [
            jnp.concatenate([by_head[0:64], zero], axis=1),
            jnp.concatenate([zero, by_head[64:128]], axis=1),
        ],
        axis=0,
    )
    window_key = jnp.concatenate([wkv_ref[r, 0, 0], wkv_ref[r, 0, 1]], axis=1)
    window_value = jnp.concatenate([wkv_ref[r, 1, 0], wkv_ref[r, 1, 1]], axis=1)

    def side(kv):
        return jnp.concatenate(
            [
                jnp.concatenate(
                    [
                        cache_ref[table_ref[0, 0, r, j], kv, 0],
                        cache_ref[table_ref[0, 0, r, j], kv, 1],
                    ],
                    axis=1,
                )
                for j in range(pages)
            ],
            axis=0,
        )

    s = lax.dot_general(query, side(0), NT, preferred_element_type=F32) * scale
    position = lax.broadcasted_iota(jnp.int32, s.shape, 1)
    s = jnp.where(position < length, s, -1e30)
    sw = lax.dot_general(query, window_key, NT, preferred_element_type=F32) * scale
    token = lax.broadcasted_iota(jnp.int32, sw.shape, 0) % 8
    place = lax.broadcasted_iota(jnp.int32, sw.shape, 1)
    sw = jnp.where(place <= token, sw, -1e30)
    top = jnp.maximum(jnp.max(s, axis=1, keepdims=True), jnp.max(sw, axis=1, keepdims=True))
    p = jnp.exp(s - top)
    pw = jnp.exp(sw - top)
    total = jnp.sum(p, axis=1, keepdims=True) + jnp.sum(pw, axis=1, keepdims=True)
    inverse = 1.0 / total
    p = (p * inverse).astype(BF16)
    pw = (pw * inverse).astype(BF16)
    out = jnp.dot(p, side(1), preferred_element_type=F32)
    out = out + jnp.dot(pw, window_value, preferred_element_type=F32)
    rows = pl.ds(pl.multiple_of(r * 8, 8), 8)
    ctx32[0:8, rows, :] = out[0:64, 0:128].reshape(8, 8, 128)
    ctx32[8:16, rows, :] = out[64:128, 128:256].reshape(8, 8, 128)


def kernel(
    len_ref,
    table_ref,
    adapter_ref,
    layer_ref,
    q_hbm,
    wkv_hbm,
    cache_hbm,
    down_hbm,
    up_hbm,
    hidden_hbm,
    wo_hbm,
    out_ref,
    cache,
    q_ref,
    wkv,
    hidden,
    down_stage,
    up_stage,
    down_all,
    up_all,
    ctx32,
    heads,
    flat,
    ctx_all,
    wbuf,
    far_send,
    far_recv,
    part,
    near_send,
    near_recv,
    own,
    z_send,
    zx_recv,
    zq_send,
    zq_recv,
    z_own,
    zq_all,
    z_all,
    delta_send,
    delta_recv,
    final,
    lsem,
    wsem,
    down_s,
    down_r,
    up_s,
    up_r,
    ctx_s,
    ctx_r,
    z_s,
    z_r,
    za_s,
    za_r,
    delta_s,
    delta_r,
    tp_s,
    tp_r,
    zx_s,
    zx_r,
    zt_s,
    zt_r,
    sec_s,
    sec_r,
):
    me = lax.axis_index("pool")
    x = lax.axis_index("tp")
    sec = lax.axis_index("section")
    mz = me // SIDE
    my = lax.rem(me, SIDE)
    adapters = layer_ref.shape[0] // 2
    start = sec * adapters

    def slot(p, r):
        return lax.rem(layer_ref[start + adapter_ref[sec, p, r]], adapters)

    def peer(k):
        dz = lax.rem(k, SIDE)
        dy = dz + k // SIDE
        return lax.rem(mz + dz, SIDE) * SIDE + lax.rem(my + dy, SIDE)

    def origin(k):
        dz = SIDE - lax.rem(k, SIDE)
        dy = dz + SIDE - k // SIDE
        return lax.rem(mz + dz, SIDE) * SIDE + lax.rem(my + dy, SIDE)

    def each(low, high, fn):
        def step(k, carry):
            fn(k)
            return carry

        lax.fori_loop(low, high, step, 0)

    def pool_copy(src, dst, ssem, rsem, k, to):
        return pltpu.make_async_remote_copy(
            src_ref=src,
            dst_ref=dst,
            send_sem=ssem.at[k],
            recv_sem=rsem.at[k],
            device_id={"pool": to},
            device_id_type=MESH,
        )

    def next_copy(src, dst, ssem, rsem, k, to):
        return pltpu.make_async_remote_copy(
            src_ref=src,
            dst_ref=dst,
            send_sem=ssem.at[k],
            recv_sem=rsem.at[k],
            device_id={"pool": to, "tp": lax.rem(x + 1, SIDE)},
            device_id_type=MESH,
        )

    def columns(ref, j):
        return ref.at[:, :, pl.ds(pl.multiple_of(j * HEAD, HEAD), HEAD)]

    held = down_hbm.shape[0]

    def pages_of(ref, j):
        return ref.at[pl.ds(j * held, held)]

    def stage_copy(ref, stage, full, k, base):
        j = peer(k)
        return pltpu.make_async_copy(columns(ref, j), stage.at[j], lsem.at[base + k])

    def own_copy(ref, full, base):
        return pltpu.make_async_copy(columns(ref, me), pages_of(full, me), lsem.at[base])

    quarter = cache.shape[0] // 4

    def cache_copy(i):
        return pltpu.make_async_copy(
            cache_hbm.at[0, 0, i * quarter : (i + 1) * quarter],
            cache.at[i * quarter : (i + 1) * quarter],
            lsem.at[32 + i],
        )

    wkv_copy = pltpu.make_async_copy(wkv_hbm.at[0, 0], wkv, lsem.at[36])
    query_copy = pltpu.make_async_copy(q_hbm.at[0, 0], q_ref, lsem.at[38])
    hidden_copy = pltpu.make_async_copy(hidden_hbm.at[0, 0], hidden, lsem.at[37])

    for k in EVEN:
        stage_copy(down_hbm, down_stage, down_all, k, 0).start()
    own_copy(down_hbm, down_all, 0).start()
    query_copy.start()
    wkv_copy.start()

    barrier = pltpu.get_barrier_semaphore()

    def greet(k):
        pl.semaphore_signal(barrier, inc=1, device_id={"pool": peer(k)}, device_id_type=MESH)

    def greet_behind(k):
        before = lax.rem(x + 3, SIDE)
        target = {"pool": peer(k), "tp": before}
        pl.semaphore_signal(barrier, inc=1, device_id=target, device_id_type=MESH)

    each(1, POOL, greet)
    each(1, POOL, greet_behind)
    for o in (1, 2, 3):
        pl.semaphore_signal(
            barrier, inc=1, device_id={"tp": lax.rem(x + o, SIDE)}, device_id_type=MESH
        )
    pl.semaphore_signal(barrier, inc=1, device_id={"section": 1 - sec}, device_id_type=MESH)
    pl.semaphore_wait(barrier, 2 * (POOL - 1) + 3 + 1)
    for i in range(4):
        cache_copy(i).start()

    def send_down(k):
        stage_copy(down_hbm, down_stage, down_all, k, 0).wait()
        pool_copy(down_stage.at[peer(k)], pages_of(down_all, me), down_s, down_r, k, peer(k)).start()

    for k in EVEN:
        send_down(k)
    own_copy(down_hbm, down_all, 0).wait()

    query_copy.wait()
    wkv_copy.wait()
    for i in range(4):
        cache_copy(i).wait()

    for k in EVEN:
        stage_copy(up_hbm, up_stage, up_all, k, 16).start()
    own_copy(up_hbm, up_all, 16).start()
    hidden_copy.start()

    def wo_copy(i):
        target = lax.rem(x + ORDER[i // 4], SIDE)
        col = target * (SIDE * TILE) + (i % 4) * TILE
        return pltpu.make_async_copy(
            wo_hbm.at[0, :, pl.ds(pl.multiple_of(col, TILE), TILE)],
            wbuf.at[i % BUFS],
            wsem.at[i % BUFS],
        )

    for i in range(BUFS):
        wo_copy(i).start()

    to = lax.broadcasted_iota(jnp.int32, (128, 128), 0)
    source = lax.broadcasted_iota(jnp.int32, (128, 128), 1)
    swap = jnp.where(source == (to % 8) * 16 + to // 8, 1.0, 0.0).astype(BF16)

    def attend_step(r, carry):
        attend_one(r, swap, len_ref, table_ref, q_ref, wkv, cache, ctx32)
        return carry

    lax.fori_loop(0, q_ref.shape[0], attend_step, 0)
    for h in range(POOL):
        block = ctx32[h].astype(BF16)
        heads[h] = block
        flat[:, h * HEAD : (h + 1) * HEAD] = block

    def send_ctx(k):
        pool_copy(heads.at[peer(k)], ctx_all.at[me], ctx_s, ctx_r, k, peer(k)).start()

    each(1, POOL, send_ctx)
    ctx_all[me] = heads[me]

    def send_up(k):
        stage_copy(up_hbm, up_stage, up_all, k, 16).wait()
        pool_copy(up_stage.at[peer(k)], pages_of(up_all, me), up_s, up_r, k, peer(k)).start()

    for k in BATCH[0]:
        send_up(k)
    own_copy(up_hbm, up_all, 16).wait()

    def wo_tile(i):
        wo_copy(i).wait()
        value = jnp.dot(flat[...], wbuf[i % BUFS], preferred_element_type=F32)
        cols = slice((i % 4) * TILE, (i % 4 + 1) * TILE)
        group = i // 4
        if group == 0:
            far_send[:, cols] = value.astype(BF16)
        elif group == 3:
            own[:, cols] = value
        else:
            part[group - 1, :, cols] = value
        if i + BUFS < 16:
            wo_copy(i + BUFS).start()

    def tp_copy(src, dst, i, step):
        return pltpu.make_async_remote_copy(
            src_ref=src,
            dst_ref=dst,
            send_sem=tp_s.at[i],
            recv_sem=tp_r.at[i],
            device_id={"tp": lax.rem(x + SIDE + step, SIDE)},
            device_id_type=MESH,
        )

    def far_copy(i, step):
        return tp_copy(far_send.at[pl.ds(i * 64, 64)], far_recv.at[i], i, step)

    def near_copy(i, half):
        rows = pl.ds(half * 64, 64)
        src, dst = near_send.at[i, rows], near_recv.at[i, rows]
        return tp_copy(src, dst, 2 + 2 * i + half, 1 - 2 * i)

    for i in range(4):
        wo_tile(i)
    far_copy(0, 1).start()
    far_copy(1, -1).start()
    for i in range(4, 8):
        wo_tile(i)
    near_send[0, 64:128] = part[0, 64:128].astype(BF16)
    near_copy(0, 1).start()

    def wait_ctx(k):
        s = origin(k)
        pool_copy(heads.at[s], ctx_all.at[s], ctx_s, ctx_r, k, s).wait_recv()

    def wait_down(k):
        s = origin(k)
        pool_copy(down_stage.at[s], pages_of(down_all, s), down_s, down_r, k, s).wait_recv()

    each(1, POOL, wait_down)

    low = lax.broadcasted_iota(jnp.int32, (32, 128), 1) < 64
    keep = own_block((32, 256))

    def gathered(ref, p, g):
        return jnp.concatenate([ref[slot(p, g * 4 + a)] for a in range(4)], axis=0)

    def down_block(p):
        pieces = []
        for g in range(4):
            pages = gathered(down_all, p, g)
            rows = ctx_all[p, g * 32 : (g + 1) * 32, :]
            wide = lax.dot_general(rows, pages, NT, preferred_element_type=F32)
            wide = jnp.where(keep, wide, 0.0)
            half = wide[:, 0:128] + wide[:, 128:256]
            pieces.append(half + pltpu.roll(half, 64, 1))
        z_send[p, 0:32, :] = jnp.where(low, pieces[0], pieces[2]).astype(BF16)
        z_send[p, 32:64, :] = jnp.where(low, pieces[1], pieces[3]).astype(BF16)


    for k in BATCH[1]:
        send_up(k)
    down_block(me)

    def arrived(k):
        wait_ctx(k)
        down_block(origin(k))

    each(1, POOL, arrived)

    def quarter_rows(ref, o):
        return ref.at[:, pl.ds(pl.multiple_of(lax.rem(x + o, SIDE) * 16, 16), 16), :]

    def line_copy(src, dst, ssem, rsem, o):
        return pltpu.make_async_remote_copy(
            src_ref=src,
            dst_ref=dst,
            send_sem=ssem.at[o - 1],
            recv_sem=rsem.at[o - 1],
            device_id={"tp": lax.rem(x + o, SIDE)},
            device_id_type=MESH,
        )

    def part_copy(o):
        return line_copy(quarter_rows(z_send, o), zx_recv.at[o - 1], zx_s, zx_r, o)

    for o in (2, 1, 3):
        part_copy(o).start()
    for i in range(8, 10):
        wo_tile(i)
    for o in (1, 2, 3):
        part_copy(o).wait_recv()
    mine = pl.ds(pl.multiple_of(x * 16, 16), 16)
    total = z_send[:, mine, :].astype(F32)
    for o in range(3):
        total = total + zx_recv[o].astype(F32)
    zq_send[...] = total.astype(BF16)

    def send_z(k):
        next_copy(zq_send.at[peer(k)], zq_recv.at[me], z_s, z_r, k, peer(k)).start()

    for k in EVEN + (0,):
        send_z(k)
    for k in BATCH[2]:
        send_up(k)
    for i in range(10, 12):
        wo_tile(i)
    near_send[1, 0:64] = part[1, 0:64].astype(BF16)
    near_copy(1, 0).start()

    def wait_z(k):
        s = origin(k)
        next_copy(zq_send.at[s], zq_recv.at[s], z_s, z_r, k, s).wait_recv()

    each(0, POOL, wait_z)
    total = zq_recv[0].astype(F32)
    for p in range(1, POOL):
        total = total + zq_recv[p].astype(F32)
    z_own[...] = total.astype(BF16)

    def send_za(k):
        next_copy(z_own, zq_all.at[me], za_s, za_r, k, peer(k)).start()

    for k in EVEN + (0,):
        send_za(k)
    for k in BATCH[3]:
        send_up(k)
    for i in range(12, 14):
        wo_tile(i)
    far_copy(0, 1).wait_recv()
    far_copy(1, -1).wait_recv()
    near_send[0, 0:64] = (part[0, 0:64] + far_recv[0].astype(F32)).astype(BF16)
    near_send[1, 64:128] = (part[1, 64:128] + far_recv[1].astype(F32)).astype(BF16)

    def wait_za(k):
        next_copy(z_own, zq_all.at[origin(k)], za_s, za_r, k, origin(k)).wait_recv()

    each(0, POOL, wait_za)

    def whole_copy(o):
        rows = quarter_rows(z_all, 2)
        return line_copy(zq_all, rows, zt_s, zt_r, o)

    def whole_wait(o):
        rows = quarter_rows(z_all, SIDE - o + 2)
        line_copy(zq_all, rows, zt_s, zt_r, o).wait_recv()

    for o in (2, 1, 3):
        whole_copy(o).start()
    held_rows = pl.ds(pl.multiple_of(lax.rem(x + 2, SIDE) * 16, 16), 16)
    z_all[:, held_rows, :] = zq_all[...]

    near_copy(0, 0).start()
    near_copy(1, 1).start()
    for i in range(14, 16):
        wo_tile(i)

    def wait_up(k):
        s = origin(k)
        pool_copy(up_stage.at[s], pages_of(up_all, s), up_s, up_r, k, s).wait_recv()

    for o in (1, 2, 3):
        whole_wait(o)
    each(1, POOL, wait_up)

    def up_block(p):
        pieces = [None] * 4
        for h in range(2):
            v = z_all[p, h * 32 : h * 32 + 32, :].astype(F32)
            turned = pltpu.roll(v, 64, 1)
            pieces[h] = jnp.where(low, v, turned)
            pieces[h + 2] = jnp.where(low, turned, v)
        for g in range(4):
            pages = gathered(up_all, p, g)
            twice = jnp.concatenate([pieces[g], pieces[g]], axis=1)
            rows = jnp.where(keep, twice, 0.0).astype(BF16)
            out = jnp.dot(rows, pages, preferred_element_type=F32)
            delta_send[p, g * 32 : (g + 1) * 32, :] = out.astype(BF16)

    def delta_copy(k, s, j):
        return pool_copy(delta_send.at[j], delta_recv.at[s], delta_s, delta_r, k, j)

    def up_and_send(k):
        up_block(peer(k))
        delta_copy(k, me, peer(k)).start()

    each(1, POOL, up_and_send)
    up_block(me)
    delta_recv[me] = delta_send[me]
    hidden_copy.wait()
    for i in range(2):
        for half in range(2):
            near_copy(i, half).wait_recv()
    own[...] = (
        own[...]
        + hidden[...].astype(F32)
        + near_recv[0].astype(F32)
        + near_recv[1].astype(F32)
    )


    def wait_delta(k):
        s = origin(k)
        delta_copy(k, s, s).wait_recv()

    def hand_copy(j):
        return pltpu.make_async_remote_copy(
            src_ref=final.at[j],
            dst_ref=out_ref.at[:, pl.ds(pl.multiple_of(j * HEAD, HEAD), HEAD)],
            send_sem=sec_s.at[j],
            recv_sem=sec_r.at[j],
            device_id={"section": 1 - sec},
            device_id_type=MESH,
        )

    def finish(j):
        value = own[:, pl.ds(pl.multiple_of(j * HEAD, HEAD), HEAD)]
        final[j] = (value + delta_recv[j].astype(F32)).astype(BF16)
        hand_copy(j).start()

    finish(me)

    def take(k):
        wait_delta(k)
        finish(origin(k))

    each(1, POOL, take)

    def drain(k):
        j = peer(k)
        pool_copy(down_stage.at[j], pages_of(down_all, me), down_s, down_r, k, j).wait_send()
        pool_copy(up_stage.at[j], pages_of(up_all, me), up_s, up_r, k, j).wait_send()
        pool_copy(heads.at[j], ctx_all.at[me], ctx_s, ctx_r, k, j).wait_send()
        delta_copy(k, me, j).wait_send()

    def drain_z(k):
        j = peer(k)
        next_copy(zq_send.at[j], zq_recv.at[me], z_s, z_r, k, j).wait_send()
        next_copy(z_own, zq_all.at[me], za_s, za_r, k, j).wait_send()

    each(1, POOL, drain)
    each(0, POOL, drain_z)
    for o in (1, 2, 3):
        part_copy(o).wait_send()
        whole_copy(o).wait_send()
    far_copy(0, 1).wait_send()
    far_copy(1, -1).wait_send()
    for i in range(2):
        for half in range(2):
            near_copy(i, half).wait_send()

    def handed(j):
        hand_copy(j).wait_send()
        hand_copy(j).wait_recv()

    each(0, POOL, handed)


def per_device(
    hidden,
    queries,
    window_key_value,
    cached_key_value,
    cached_length,
    request_page_table,
    request_adapter,
    layer_page_slot,
    wo,
    adapter_down,
    adapter_up,
):
    rows = queries.shape[2] * queries.shape[3]
    width = hidden.shape[3]
    pages = adapter_down.shape[:2] + (HEAD,)
    smem = pl.BlockSpec(memory_space=pltpu.SMEM)
    vmem = pl.BlockSpec(memory_space=pltpu.VMEM)
    hbm = pl.BlockSpec(memory_space=pl.ANY)
    dma = pltpu.SemaphoreType.DMA
    handed = pl.pallas_call(
        kernel,
        out_shape=jax.ShapeDtypeStruct((rows, width), BF16),
        in_specs=[smem, smem, smem, smem, hbm, hbm, hbm, hbm, hbm, hbm, hbm],
        out_specs=vmem,
        scratch_shapes=[
            pltpu.VMEM(cached_key_value.shape[2:], BF16),
            pltpu.VMEM(queries.shape[2:], BF16),
            pltpu.VMEM(window_key_value.shape[2:], BF16),
            pltpu.VMEM((rows, width), BF16),
            pltpu.VMEM((POOL,) + pages, BF16),
            pltpu.VMEM((POOL,) + pages, BF16),
            pltpu.VMEM((POOL * pages[0],) + pages[1:], BF16),
            pltpu.VMEM((POOL * pages[0],) + pages[1:], BF16),
            pltpu.VMEM((POOL, rows, HEAD), F32),
            pltpu.VMEM((POOL, rows, HEAD), BF16),
            pltpu.VMEM((rows, width), BF16),
            pltpu.VMEM((POOL, rows, HEAD), BF16),
            pltpu.VMEM((BUFS, width, TILE), BF16),
            pltpu.VMEM((rows, width), BF16),
            pltpu.VMEM((2, 64, width), BF16),
            pltpu.VMEM((2, rows, width), F32),
            pltpu.VMEM((2, rows, width), BF16),
            pltpu.VMEM((2, rows, width), BF16),
            pltpu.VMEM((rows, width), F32),
            pltpu.VMEM((POOL, 64, HEAD), BF16),
            pltpu.VMEM((3, POOL, 16, HEAD), BF16),
            pltpu.VMEM((POOL, 16, HEAD), BF16),
            pltpu.VMEM((POOL, 16, HEAD), BF16),
            pltpu.VMEM((16, HEAD), BF16),
            pltpu.VMEM((POOL, 16, HEAD), BF16),
            pltpu.VMEM((POOL, 64, HEAD), BF16),
            pltpu.VMEM((POOL, rows, HEAD), BF16),
            pltpu.VMEM((POOL, rows, HEAD), BF16),
            pltpu.VMEM((POOL, rows, HEAD), BF16),
            dma((40,)),
            dma((BUFS,)),
            dma((POOL,)),
            dma((POOL,)),
            dma((POOL,)),
            dma((POOL,)),
            dma((POOL,)),
            dma((POOL,)),
            dma((POOL,)),
            dma((POOL,)),
            dma((POOL,)),
            dma((POOL,)),
            dma((POOL,)),
            dma((POOL,)),
            dma((6,)),
            dma((6,)),
            dma((3,)),
            dma((3,)),
            dma((3,)),
            dma((3,)),
            dma((POOL,)),
            dma((POOL,)),
        ],
        compiler_params=pltpu.CompilerParams(
            collective_id=0, has_side_effects=True, vmem_limit_bytes=60 * 2**20
        ),
        name="relay_layer",
    )(
        cached_length,
        request_page_table,
        request_adapter,
        layer_page_slot,
        queries,
        window_key_value,
        cached_key_value,
        adapter_down,
        adapter_up,
        hidden,
        wo,
    )
    return handed[None, None]


def solution(mesh):
    return jax.shard_map(
        per_device,
        mesh=mesh,
        in_specs=(
            P("section", "pool", None, "tp"),
            P("section", "pool", None, None, "tp", None),
            P("section", "pool", None, None, "tp", None, None),
            P("section", "pool", None, None, "tp", None, None),
            P("section", "pool", None),
            P("section", "pool", None, None),
            P(),
            P(),
            P("section", "tp", None),
            P(("section", "pool"), None, "tp"),
            P(("section", "pool"), None, "tp"),
        ),
        out_specs=P("section", "pool", None, "tp"),
        check_vma=False,
    )
```
